32 devices in a mesh: section: 4 (over x, core), fsdp: 8 (over z, y).
Axes of the slice: x: 2, y: 2, z: 4, core: 2. Of those that a mesh axis runs over, the one named last changes fastest.
Arguments:
- tokens: bfloat16 [4, 2, 1024, 8192], P('section', None, 'fsdp'), may hold values from -6 to 6
- queries: bfloat16 [4, 2, 1024, 4096], P('section', None, 'fsdp'), may hold values from -200 to 200
- gains: bfloat16 [4, 8192], P('section'), may hold values from 0.5 to 1.5
- key_weight: bfloat16 [4, 8192, 512], P('section', 'fsdp'), may hold values from -0.0625 to 0.0625
- value_weight: bfloat16 [4, 8192, 512], P('section', 'fsdp'), may hold values from -0.0625 to 0.0625
- lengths: int32 [2, 16], replicated, may hold values from 1 to 128, 1024 in all within a row
Outputs:
- attended: bfloat16 [4, 2, 1024, 4096], P('section', None, 'fsdp')
The draws below stay inside these ranges and needn't reach their ends.
Inputs may be any that keep to these rules, and one draw needn't show every extreme that they name: `lengths`: each row sums to 1024; some document has exactly 128 tokens.
All inputs are finite; a program needn't handle non-finite values.
Results may differ from the reference program's by a relative error of at most 0.012.
The reference program's roundings to bfloat16 on the way (of `normed`) count: a program that leaves them out, or rounds other values in their place, can miss the bound.
Values may be sent and summed in bfloat16 or wider, within the bound.
A program may use at most 128 MiB of HBM per device.

```python
import math
import jax
import jax.numpy as jnp
import numpy as np
from jax import lax

D = 8192
KV_HEADS = 4
Q_HEADS = 32
HEAD = 128
MICRO = 2
TOK_DEV = 128
TOKENS = 1024
DOCS = 16
LAYERS = 4


def draw_queries(key, part):
    shape = (LAYERS, MICRO, TOKENS, Q_HEADS * HEAD)
    normal_part = jax.random.normal(jax.random.fold_in(key, 11), shape, jnp.float32)
    drawn = jnp.clip(normal_part, -6.0, 6.0)
    return drawn.astype(jnp.bfloat16)


def block_levels(stream_key, extent, pieces, low, high):
    def one(position, blocks):
        draws = jax.random.uniform(jax.random.fold_in(jax.random.fold_in(stream_key, 6), position), (blocks,), jnp.float32, low / len(pieces), high / len(pieces))
        return jnp.repeat(jnp.exp(draws), extent[position] // blocks).reshape((-1,) + (1,) * (len(extent) - position - 1))

    factor_of = one(*pieces[0])
    for cut in pieces[1:]:
        factor_of = factor_of * one(*cut)
    return factor_of


def profile(number_of, total, most, skew):
    portions = [(1 << 20) // math.isqrt(standing ** skew) + 1 for standing in range(2, number_of + 1)]
    spare, holding = total - most - (number_of - 1), [1] * (number_of - 1)
    while spare > 0:
        movable = [i for i in range(number_of - 1) if holding[i] < most]
        mass, remaining = sum([portions[i] for i in movable]), spare
        for i in movable:
            addition = min(most - holding[i], max(1, remaining * portions[i] // mass), spare)
            holding[i] = holding[i] + addition
            spare = spare - addition
    return np.array([most] + holding)


def ragged_sizes(rng, amount, total, most, slope):
    if amount == 2:
        one = jax.random.randint(rng, (), max(1, total - most), min(most, total - 1) + 1)
        return jnp.stack([one, total - one])
    sizes = jnp.asarray(profile(amount, total, most, slope), jnp.int32)
    couples = (amount - 1) // 2
    source_of, taker = sizes[1:1 + 2 * couples:2], sizes[2:2 + 2 * couples:2]
    room = jnp.minimum(source_of - 1, most - taker)
    passed = jax.random.randint(jax.random.fold_in(rng, 1), (couples,), 0, 1 << 20) % (room + 1)
    sizes = sizes.at[1:1 + 2 * couples:2].set(source_of - passed).at[2:2 + 2 * couples:2].set(taker + passed)
    return sizes[jax.random.permutation(jax.random.fold_in(rng, 2), amount)]


def scatter_about(own_key, dims, width, most, pieces=(), kind=jnp.bfloat16):
    values = jax.random.normal(own_key, dims, jnp.float32) * width
    if len(pieces) > 0:
        values = block_levels(own_key, dims, pieces, -0.22, 0.18) * values
    return jnp.clip(values, min=-most, max=most).astype(kind)


def setup_inputs(seed: int = 0) -> dict:
    key_list = jax.random.split(jax.random.key(seed), 7)
    return {
        "tokens": scatter_about(key_list[0], (LAYERS, MICRO, TOKENS, D), 1.0, 6.0, ((0, 4), (2, 8))),
        "queries": draw_queries(jax.random.fold_in(key_list[6], 71), 0),
        "gains": jnp.clip(1.0 + 0.1 * jax.random.normal(key_list[2], (LAYERS, D), jnp.float32), 0.5, 1.5).astype(jnp.bfloat16),
        "key_weight": scatter_about(key_list[3], (LAYERS, D, KV_HEADS * HEAD), D ** -0.5, 0.0625, ((0, 4), (1, 8))),
        "value_weight": scatter_about(key_list[4], (LAYERS, D, KV_HEADS * HEAD), D ** -0.5, 0.0625, ((0, 4), (1, 8))),
        "lengths": jax.vmap(lambda own: ragged_sizes(own, DOCS, TOKENS, TOK_DEV, 2))(jax.random.split(key_list[5], MICRO)).reshape((MICRO, DOCS)).astype(jnp.int32),
    }


def rms_norm(hidden, gain_row):
    widened = hidden.astype(jnp.float32)
    inverse_rms = lax.rsqrt(lax.optimization_barrier(jnp.mean(widened * widened, axis=-1, keepdims=True)) + 1e-05)
    return (widened * inverse_rms * gain_row.astype(jnp.float32)).astype(jnp.bfloat16)

def document_ids(length_row, positions):
    bounds = jnp.cumsum(length_row.astype(jnp.int32))
    return lax.optimization_barrier(jnp.sum((bounds[None, :] <= positions[:, None]).astype(jnp.int32), axis=1))

def block_attend(query_rows, key_rows, value_rows, query_pos, key_pos, query_doc, key_doc):
    query_count = query_rows.shape[0]
    key_count = key_rows.shape[0]
    kv_count = key_rows.shape[1] // HEAD
    group_count = query_rows.shape[1] // (kv_count * HEAD)
    query_heads = query_rows.reshape(query_count, kv_count, group_count, HEAD).astype(jnp.float32)
    key_heads = key_rows.reshape(key_count, kv_count, HEAD).astype(jnp.float32)
    value_heads = value_rows.reshape(key_count, kv_count, HEAD).astype(jnp.float32)
    scores = jnp.einsum('tkgd,skd->kgts', query_heads, key_heads) * HEAD ** (-0.5)
    allowed = (key_doc[None, :] == query_doc[:, None]) & (key_pos[None, :] <= query_pos[:, None]) & (key_pos[None, :] >= 0)
    scores = jnp.where(allowed, scores, -1e+30)
    maxima = lax.optimization_barrier(jnp.max(scores, axis=-1, keepdims=True))
    exponent = jnp.where(allowed, jnp.exp(scores - maxima), 0.0)
    totals = lax.optimization_barrier(jnp.sum(exponent, axis=-1, keepdims=True))
    softmax_rows = (exponent / totals).astype(jnp.bfloat16)
    mixed = jnp.einsum('kgts,skd->tkgd', softmax_rows.astype(jnp.float32), value_heads)
    return mixed.reshape(query_count, kv_count * group_count * HEAD).astype(jnp.bfloat16)

def attend_all(query_all, key_all, value_all, length_row):
    block_count = TOKENS // TOK_DEV
    zero_rows = jnp.zeros((TOK_DEV, key_all.shape[1]), jnp.bfloat16)
    padded_keys = jnp.concatenate([zero_rows, key_all], axis=0)
    padded_values = jnp.concatenate([zero_rows, value_all], axis=0)

    def attend_block(block_index):
        block_start = (block_index * TOK_DEV).astype(jnp.int32)
        query_rows = lax.dynamic_slice_in_dim(query_all, block_start, TOK_DEV, 0)
        key_rows = lax.dynamic_slice_in_dim(padded_keys, block_start, 2 * TOK_DEV, 0)
        value_rows = lax.dynamic_slice_in_dim(padded_values, block_start, 2 * TOK_DEV, 0)
        query_pos = block_start + jnp.arange(TOK_DEV, dtype=jnp.int32)
        key_pos = block_start - TOK_DEV + jnp.arange(2 * TOK_DEV, dtype=jnp.int32)
        return block_attend(query_rows, key_rows, value_rows, query_pos, key_pos, document_ids(length_row, query_pos), document_ids(length_row, key_pos))
    blocks_out = lax.map(attend_block, jnp.arange(block_count, dtype=jnp.int32))
    return blocks_out.reshape(TOKENS, query_all.shape[1])

def reference(tokens, queries, gains, key_weight, value_weight, lengths):
    results = []
    for slot_index in range(MICRO):
        per_layer = []
        for layer_index in range(LAYERS):
            normed = rms_norm(tokens[layer_index, slot_index], gains[layer_index])
            key_all = jnp.dot(normed, key_weight[layer_index], preferred_element_type=jnp.float32).astype(jnp.bfloat16)
            value_all = jnp.dot(normed, value_weight[layer_index], preferred_element_type=jnp.float32).astype(jnp.bfloat16)
            per_layer.append(attend_all(queries[layer_index, slot_index], key_all, value_all, lengths[slot_index]))
        results.append(jnp.stack(per_layer))
    return jnp.stack(results, axis=1)
```

```python
import functools

import jax
import jax.numpy as jnp
from jax import lax
from jax.experimental import pallas as pl
from jax.experimental.pallas import tpu as pltpu
from jax.sharding import PartitionSpec as P

HEAD = 128
AXIS = "fsdp"


def kernel(
    n,
    x_hbm, q_hbm, gain_ref, kw_hbm, vw_hbm, len_ref, o_hbm,
    x_v, q_v, o_v, wbuf, xs, sx, part_s, part_r, own_acc, kv, prior, start_s,
    lw_sem, lx_sem, lq_sem, lo_sem,
    ws_sem, wr_sem, ys_sem, yr_sem, xs_sem, xr_sem, ps_sem, pr_sem, ks_sem, kr_sem,
):
    slots, tok, depth = x_v.shape
    chunks, groups, _, rows, _ = wbuf.shape
    wide = 2 * rows
    total = slots * tok
    q_per_kv = q_v.shape[2] // (chunks * HEAD)
    me = lax.axis_index(AXIS)
    bit = me % 2
    cls = (me // 2) % 2
    grp = me // 4
    y_peer = me + 1 - 2 * bit
    z_peer = me + 2 - 4 * cls
    right = lax.rem(me + 1, n)
    left = lax.rem(me + n - 1, n)
    others = [lax.rem(grp + d, groups) for d in range(1, groups)]

    def dev(g):
        return g * 4 + cls * 2 + bit

    def load_w(c):
        cols = pl.ds(c * HEAD, HEAD)
        return [
            pltpu.make_async_copy(
                w.at[0, :, cols], wbuf.at[c, grp, bit, :, pl.ds(i * HEAD, HEAD)], lw_sem.at[c, i]
            )
            for i, w in enumerate((kw_hbm, vw_hbm))
        ]

    x_loads = [pltpu.make_async_copy(x_hbm.at[0, s], x_v.at[s], lx_sem.at[s]) for s in range(slots)]
    q_load = pltpu.make_async_copy(q_hbm.at[0], q_v, lq_sem)
    w_loads = [load_w(c) for c in range(chunks)]
    for copy in w_loads[0] + x_loads:
        copy.start()
    for c in range(1, chunks):
        for copy in w_loads[c]:
            copy.start()
    q_load.start()

    prior[...] = jnp.zeros_like(prior)

    barrier = pltpu.get_barrier_semaphore()
    peers = [y_peer, z_peer, right, left] + [dev(g) for g in others]
    for peer in peers:
        pl.semaphore_signal(barrier, inc=1, device_id={AXIS: peer}, device_id_type=pl.DeviceIdType.MESH)
    pl.semaphore_wait(barrier, len(peers))

    def remote(src, dst, send, recv, peer):
        return pltpu.make_async_remote_copy(
            src_ref=src, dst_ref=dst, send_sem=send, recv_sem=recv,
            device_id={AXIS: peer}, device_id_type=pl.DeviceIdType.MESH,
        )

    def w_copy(c, source_grp, index_grp, peer):
        block = wbuf.at[c, source_grp, bit]
        return remote(block, block, ws_sem.at[c, index_grp], wr_sem.at[c, source_grp], peer)

    def y_copy(c, g, side):
        block = wbuf.at[c, g, side]
        return remote(block, block, ys_sem.at[c, g], yr_sem.at[c, g], y_peer)

    def send_w(c):
        for copy in w_loads[c]:
            copy.wait()
        for g in others:
            w_copy(c, grp, g, dev(g)).start()
        y_copy(c, grp, bit).start()

    def x_copy(s, g):
        return remote(
            sx.at[g, pl.ds(s * tok, tok)], xs.at[g, pl.ds(total + s * tok, tok)],
            xs_sem.at[s, g], xr_sem.at[s, g], z_peer,
        )

    def p_copy(c):
        return remote(part_s.at[c], part_r.at[c], ps_sem.at[c], pr_sem.at[c], z_peer)

    def k_copy(c):
        return remote(kv.at[c], prior.at[c], ks_sem.at[c], kr_sem.at[c], right)

    send_w(0)

    block_rows = 16

    def norm_block(s, r):
        here = pl.ds(pl.multiple_of(r * block_rows, block_rows), block_rows)
        there = pl.ds(pl.multiple_of(s * tok + r * block_rows, block_rows), block_rows)
        squares = jnp.zeros((block_rows, 1), jnp.float32)
        step = 2 * wide
        for i in range(depth // step):
            piece = x_v[s, here, i * step:(i + 1) * step].astype(jnp.float32)
            squares = squares + jnp.sum(piece * piece, axis=-1, keepdims=True)
        inverse = lax.rsqrt(squares / depth + 1e-05)
        for g in range(groups):
            for mine in (True, False):
                first = (4 * g + 2 * (cls if mine else 1 - cls)) * rows
                cols = pl.ds(pl.multiple_of(first, HEAD), wide)
                value = x_v[s, here, cols].astype(jnp.float32) * inverse
                value = (value * gain_ref[0:1, cols].astype(jnp.float32)).astype(jnp.bfloat16)
                if mine:
                    xs[g, there, :] = value
                else:
                    sx[g, there, :] = value

    for s in range(slots):
        x_loads[s].wait()

        def norm_step(r, carry, s=s):
            norm_block(s, r)
            return carry

        lax.fori_loop(0, tok // block_rows, norm_step, 0)
        for g in range(groups):
            x_copy(s, g).start()

    for c in range(1, chunks):
        send_w(c)

    docs = len_ref.shape[1]
    rowi = lax.broadcasted_iota(jnp.int32, (docs, docs), 0)
    coli = lax.broadcasted_iota(jnp.int32, (docs, docs), 1)
    pos = lax.broadcasted_iota(jnp.int32, (tok, 1), 0) + me * tok
    for s in range(slots):
        lens = jnp.broadcast_to(len_ref[s:s + 1, :], (docs, docs))
        bounds = jnp.sum(jnp.where(coli <= rowi, lens, 0), axis=1, keepdims=True)
        bound_row = jnp.sum(jnp.where(coli == rowi, bounds, 0), axis=0, keepdims=True)
        start = jnp.max(jnp.where(bound_row <= pos, bound_row, 0), axis=1, keepdims=True)
        start_s[s] = jnp.broadcast_to(start, (tok, HEAD))
    q_load.wait()

    def forward(c):
        for g in others:
            w_copy(c, g, g, dev(g)).wait_recv()
            y_copy(c, g, bit).start()

    def project(c, lo):
        acc = jnp.zeros((total, 2 * HEAD), jnp.float32)
        for g in range(groups):
            acc = acc + jnp.dot(
                xs[g, lo:lo + total, :], wbuf[c, g].reshape(wide, 2 * HEAD),
                preferred_element_type=jnp.float32,
            )
        return acc

    def stage_a(c):
        for g in range(groups):
            y_copy(c, g, 1 - bit).wait_recv()
        if c == 0:
            for s in range(slots):
                for g in range(groups):
                    x_copy(s, g).wait_recv()
        part_s[c] = project(c, total)
        p_copy(c).start()
        own_acc[c] = project(c, 0)

    def stage_b(c):
        p_copy(c).wait_recv()
        kv[c] = (own_acc[c] + part_r[c]).astype(jnp.bfloat16)

        @pl.when(me < n - 1)
        def _():
            k_copy(c).start()

    key_pos = lax.broadcasted_iota(jnp.int32, (tok, 2 * tok), 1) + (me - 1) * tok
    query_pos = lax.broadcasted_iota(jnp.int32, (tok, 2 * tok), 0) + me * tok

    def out_copy(c):
        cols = pl.ds(c * q_per_kv * HEAD, q_per_kv * HEAD)
        return pltpu.make_async_copy(o_v.at[:, :, cols], o_hbm.at[0, :, :, cols], lo_sem.at[c])

    def stage_c(c):
        @pl.when(me > 0)
        def _():
            k_copy(c).wait_recv()

        for s in range(slots):
            here = slice(s * tok, (s + 1) * tok)
            keys = jnp.concatenate([prior[c, here, 0:HEAD], kv[c, here, 0:HEAD]], axis=0)
            values = jnp.concatenate([prior[c, here, HEAD:], kv[c, here, HEAD:]], axis=0)
            allowed = (key_pos >= start_s[s][:, 0:1]) & (key_pos <= query_pos)

            def head_step(h, carry, s=s, keys=keys, values=values, allowed=allowed):
                cols = pl.ds(pl.multiple_of((c * q_per_kv + h) * HEAD, HEAD), HEAD)
                scores = lax.dot_general(
                    q_v[s, :, cols], keys, (((1,), (1,)), ((), ())),
                    preferred_element_type=jnp.float32,
                ) * HEAD ** (-0.5)
                scores = jnp.where(allowed, scores, -1e30)
                maxima = jnp.max(scores, axis=-1, keepdims=True)
                exponent = jnp.where(allowed, jnp.exp(scores - maxima), 0.0)
                sums = jnp.sum(exponent, axis=-1, keepdims=True)
                soft = (exponent / sums).astype(jnp.bfloat16)
                mixed = jnp.dot(soft, values, preferred_element_type=jnp.float32)
                o_v[s, :, cols] = mixed.astype(jnp.bfloat16)
                return carry

            lax.fori_loop(0, q_per_kv, head_step, 0, unroll=2)
        out_copy(c).start()

    for step in range(chunks + 4):
        if step < chunks:
            forward(step)
        if 1 <= step <= chunks:
            stage_a(step - 1)
        if 2 <= step <= chunks + 1:
            stage_b(step - 2)
        if 3 <= step <= chunks + 2:
            stage_c(step - 3)

    for c in range(chunks):
        out_copy(c).wait()
        for g in others:
            w_copy(c, grp, g, dev(g)).wait_send()
        for g in range(groups):
            y_copy(c, g, bit).wait_send()
        p_copy(c).wait_send()

        @pl.when(me < n - 1)
        def _(c=c):
            k_copy(c).wait_send()

    for s in range(slots):
        for g in range(groups):
            x_copy(s, g).wait_send()


def body(tokens, queries, gains, key_weight, value_weight, lengths):
    n = lax.axis_size(AXIS)
    _, slots, tok, depth = tokens.shape
    _, rows, key_width = key_weight.shape
    chunks = key_width // HEAD
    groups = n // 4
    total = slots * tok
    bf, f32 = jnp.bfloat16, jnp.float32
    any_spec = pl.BlockSpec(memory_space=pl.ANY)
    vmem_spec = pl.BlockSpec(memory_space=pltpu.VMEM)
    dma = pltpu.SemaphoreType.DMA
    return pl.pallas_call(
        functools.partial(kernel, n),
        out_shape=jax.ShapeDtypeStruct(queries.shape, bf),
        in_specs=[any_spec, any_spec, vmem_spec, any_spec, any_spec, vmem_spec],
        out_specs=any_spec,
        scratch_shapes=[
            pltpu.VMEM((slots, tok, depth), bf),
            pltpu.VMEM(queries.shape[1:], bf),
            pltpu.VMEM(queries.shape[1:], bf),
            pltpu.VMEM((chunks, groups, 2, rows, 2 * HEAD), bf),
            pltpu.VMEM((groups, 2 * total, 2 * rows), bf),
            pltpu.VMEM((groups, total, 2 * rows), bf),
            pltpu.VMEM((chunks, total, 2 * HEAD), f32),
            pltpu.VMEM((chunks, total, 2 * HEAD), f32),
            pltpu.VMEM((chunks, total, 2 * HEAD), f32),
            pltpu.VMEM((chunks, total, 2 * HEAD), bf),
            pltpu.VMEM((chunks, total, 2 * HEAD), bf),
            pltpu.VMEM((slots, tok, HEAD), jnp.int32),
            dma((chunks, 2)), dma((slots,)), dma, dma((chunks,)),
            dma((chunks, groups)), dma((chunks, groups)),
            dma((chunks, groups)), dma((chunks, groups)),
            dma((slots, groups)), dma((slots, groups)),
            dma((chunks,)), dma((chunks,)), dma((chunks,)), dma((chunks,)),
        ],
        compiler_params=pltpu.CompilerParams(
            collective_id=0, has_side_effects=True, vmem_limit_bytes=60 * 1024 * 1024
        ),
    )(tokens, queries, gains, key_weight, value_weight, lengths)


def solution(mesh):
    return jax.shard_map(
        body,
        mesh=mesh,
        in_specs=(
            P("section", None, "fsdp", None),
            P("section", None, "fsdp", None),
            P("section", None),
            P("section", "fsdp", None),
            P("section", "fsdp", None),
            P(),
        ),
        out_specs=P("section", None, "fsdp", None),
        check_vma=False,
    )
```

```python
import functools

import jax
import jax.numpy as jnp
from jax import lax
from jax.experimental import pallas as pl
from jax.experimental.pallas import tpu as pltpu
from jax.sharding import PartitionSpec as P

HEAD = 128
AXIS = "fsdp"


def kernel(
    n,
    x_hbm, q_hbm, gain_ref, kw_hbm, vw_hbm, len_ref, o_hbm,
    x_v, q_v, o_v, wbuf, xs, sx, part_s, part_r, own_acc, kv, prior, start_s,
    lw_sem, lx_sem, lq_sem, lo_sem,
    ws_sem, wr_sem, ys_sem, yr_sem, xs_sem, xr_sem, ps_sem, pr_sem, ks_sem, kr_sem,
):
    slots, tok, depth = x_v.shape
    chunks, groups, _, rows, _ = wbuf.shape
    wide = 2 * rows
    total = slots * tok
    q_per_kv = q_v.shape[2] // (chunks * HEAD)
    me = lax.axis_index(AXIS)
    bit = me % 2
    cls = (me // 2) % 2
    grp = me // 4
    y_peer = me + 1 - 2 * bit
    z_peer = me + 2 - 4 * cls
    right = lax.rem(me + 1, n)
    left = lax.rem(me + n - 1, n)
    others = [lax.rem(grp + d, groups) for d in range(1, groups)]

    def dev(g):
        return g * 4 + cls * 2 + bit

    def load_w(c):
        cols = pl.ds(c * HEAD, HEAD)
        return [
            pltpu.make_async_copy(
                w.at[0, :, cols], wbuf.at[c, grp, bit, :, pl.ds(i * HEAD, HEAD)], lw_sem.at[c, i]
            )
            for i, w in enumerate((kw_hbm, vw_hbm))
        ]

    x_loads = [pltpu.make_async_copy(x_hbm.at[0, s], x_v.at[s], lx_sem.at[s]) for s in range(slots)]
    q_load = pltpu.make_async_copy(q_hbm.at[0], q_v, lq_sem)
    w_loads = [load_w(c) for c in range(chunks)]
    for copy in w_loads[0] + x_loads:
        copy.start()
    for c in range(1, chunks):
        for copy in w_loads[c]:
            copy.start()
    q_load.start()

    prior[...] = jnp.zeros_like(prior)

    barrier = pltpu.get_barrier_semaphore()
    peers = [y_peer, z_peer, right, left] + [dev(g) for g in others]
    for peer in peers:
        pl.semaphore_signal(barrier, inc=1, device_id={AXIS: peer}, device_id_type=pl.DeviceIdType.MESH)
    pl.semaphore_wait(barrier, len(peers))

    def remote(src, dst, send, recv, peer):
        return pltpu.make_async_remote_copy(
            src_ref=src, dst_ref=dst, send_sem=send, recv_sem=recv,
            device_id={AXIS: peer}, device_id_type=pl.DeviceIdType.MESH,
        )

    def w_copy(c, source_grp, index_grp, peer):
        block = wbuf.at[c, source_grp, bit]
        return remote(block, block, ws_sem.at[c, index_grp], wr_sem.at[c, source_grp], peer)

    def y_copy(c, g, side):
        block = wbuf.at[c, g, side]
        return remote(block, block, ys_sem.at[c, g], yr_sem.at[c, g], y_peer)

    outer = cls == grp % 2

    def send_w(c):
        for copy in w_loads[c]:
            copy.wait()
        for g in others:
            w_copy(c, grp, g, dev(g)).start()
        y_copy(c, grp, bit).start()

    def x_copy(s, g):
        return remote(
            sx.at[g, pl.ds(s * tok, tok)], xs.at[g, pl.ds(total + s * tok, tok)],
            xs_sem.at[s, g], xr_sem.at[s, g], z_peer,
        )

    def p_copy(c):
        return remote(part_s.at[c], part_r.at[c], ps_sem.at[c], pr_sem.at[c], z_peer)

    def k_copy(c):
        return remote(kv.at[c], prior.at[c], ks_sem.at[c], kr_sem.at[c], right)

    send_w(0)

    block_rows = 16

    def norm_block(s, r):
        here = pl.ds(pl.multiple_of(r * block_rows, block_rows), block_rows)
        there = pl.ds(pl.multiple_of(s * tok + r * block_rows, block_rows), block_rows)
        squares = jnp.zeros((block_rows, 1), jnp.float32)
        step = 2 * wide
        for i in range(depth // step):
            piece = x_v[s, here, i * step:(i + 1) * step].astype(jnp.float32)
            squares = squares + jnp.sum(piece * piece, axis=-1, keepdims=True)
        inverse = lax.rsqrt(squares / depth + 1e-05)
        for g in range(groups):
            for mine in (True, False):
                first = (4 * g + 2 * (cls if mine else 1 - cls)) * rows
                cols = pl.ds(pl.multiple_of(first, HEAD), wide)
                value = x_v[s, here, cols].astype(jnp.float32) * inverse
                value = (value * gain_ref[0:1, cols].astype(jnp.float32)).astype(jnp.bfloat16)
                if mine:
                    xs[g, there, :] = value
                else:
                    sx[g, there, :] = value

    for s in range(slots):
        x_loads[s].wait()

        def norm_step(r, carry, s=s):
            norm_block(s, r)
            return carry

        lax.fori_loop(0, tok // block_rows, norm_step, 0)
        @pl.when(outer)
        def _(s=s):
            for g in range(groups):
                x_copy(s, g).start()

    for c in range(1, chunks):
        send_w(c)

    docs = len_ref.shape[1]
    rowi = lax.broadcasted_iota(jnp.int32, (docs, docs), 0)
    coli = lax.broadcasted_iota(jnp.int32, (docs, docs), 1)
    pos = lax.broadcasted_iota(jnp.int32, (tok, 1), 0) + me * tok
    for s in range(slots):
        lens = jnp.broadcast_to(len_ref[s:s + 1, :], (docs, docs))
        bounds = jnp.sum(jnp.where(coli <= rowi, lens, 0), axis=1, keepdims=True)
        bound_row = jnp.sum(jnp.where(coli == rowi, bounds, 0), axis=0, keepdims=True)
        start = jnp.max(jnp.where(bound_row <= pos, bound_row, 0), axis=1, keepdims=True)
        start_s[s] = jnp.broadcast_to(start, (tok, HEAD))
    q_load.wait()

    @pl.when(jnp.logical_not(outer))
    def _():
        for c in range(chunks):
            for g in others:
                w_copy(c, grp, g, dev(g)).wait_send()
        for s in range(slots):
            for g in range(groups):
                x_copy(s, g).start()

    def forward(c):
        for g in others:
            w_copy(c, g, g, dev(g)).wait_recv()
            y_copy(c, g, bit).start()

    def project(c, lo):
        acc = jnp.zeros((total, 2 * HEAD), jnp.float32)
        for g in range(groups):
            acc = acc + jnp.dot(
                xs[g, lo:lo + total, :], wbuf[c, g].reshape(wide, 2 * HEAD),
                preferred_element_type=jnp.float32,
            )
        return acc

    def own_rows(c):
        own_acc[c] = project(c, 0)

    def y_wait(c):
        for g in range(groups):
            y_copy(c, g, 1 - bit).wait_recv()

    @pl.when(outer)
    def _():
        for c in range(chunks):
            forward(c)
        for c in range(chunks):
            y_wait(c)
            own_rows(c)

    def stage_a(c):
        @pl.when(jnp.logical_not(outer))
        def _():
            if c == 0:
                forward(0)
            if c + 1 < chunks:
                forward(c + 1)
            y_wait(c)

        if c == 0:
            for s in range(slots):
                for g in range(groups):
                    x_copy(s, g).wait_recv()
        part_s[c] = project(c, total)
        p_copy(c).start()

        @pl.when(jnp.logical_not(outer))
        def _():
            own_rows(c)

    def stage_b(c):
        p_copy(c).wait_recv()
        kv[c] = (own_acc[c] + part_r[c]).astype(jnp.bfloat16)

        @pl.when(me < n - 1)
        def _():
            k_copy(c).start()

    key_pos = lax.broadcasted_iota(jnp.int32, (tok, 2 * tok), 1) + (me - 1) * tok
    query_pos = lax.broadcasted_iota(jnp.int32, (tok, 2 * tok), 0) + me * tok

    def out_copy(c):
        cols = pl.ds(c * q_per_kv * HEAD, q_per_kv * HEAD)
        return pltpu.make_async_copy(o_v.at[:, :, cols], o_hbm.at[0, :, :, cols], lo_sem.at[c])

    def stage_c(c):
        @pl.when(me > 0)
        def _():
            k_copy(c).wait_recv()

        for s in range(slots):
            here = slice(s * tok, (s + 1) * tok)
            keys = jnp.concatenate([prior[c, here, 0:HEAD], kv[c, here, 0:HEAD]], axis=0)
            values = jnp.concatenate([prior[c, here, HEAD:], kv[c, here, HEAD:]], axis=0)
            allowed = (key_pos >= start_s[s][:, 0:1]) & (key_pos <= query_pos)

            def head_step(h, carry, s=s, keys=keys, values=values, allowed=allowed):
                cols = pl.ds(pl.multiple_of((c * q_per_kv + h) * HEAD, HEAD), HEAD)
                scores = lax.dot_general(
                    q_v[s, :, cols], keys, (((1,), (1,)), ((), ())),
                    preferred_element_type=jnp.float32,
                ) * HEAD ** (-0.5)
                scores = jnp.where(allowed, scores, -1e30)
                maxima = jnp.max(scores, axis=-1, keepdims=True)
                exponent = jnp.where(allowed, jnp.exp(scores - maxima), 0.0)
                sums = jnp.sum(exponent, axis=-1, keepdims=True)
                soft = (exponent / sums).astype(jnp.bfloat16)
                mixed = jnp.dot(soft, values, preferred_element_type=jnp.float32)
                o_v[s, :, cols] = mixed.astype(jnp.bfloat16)
                return carry

            lax.fori_loop(0, q_per_kv, head_step, 0, unroll=True)
        out_copy(c).start()

    for c in range(chunks - 1):
        stage_a(c)
    stage_b(0)
    stage_b(1)
    stage_a(chunks - 1)
    for c in range(2, chunks):
        stage_c(c - 2)
        stage_b(c)
    stage_c(chunks - 2)
    stage_c(chunks - 1)

    for c in range(chunks):
        out_copy(c).wait()
        @pl.when(outer)
        def _(c=c):
            for g in others:
                w_copy(c, grp, g, dev(g)).wait_send()

        for g in range(groups):
            y_copy(c, g, bit).wait_send()
        p_copy(c).wait_send()

        @pl.when(me < n - 1)
        def _(c=c):
            k_copy(c).wait_send()

    for s in range(slots):
        for g in range(groups):
            x_copy(s, g).wait_send()


def body(tokens, queries, gains, key_weight, value_weight, lengths):
    n = lax.axis_size(AXIS)
    _, slots, tok, depth = tokens.shape
    _, rows, key_width = key_weight.shape
    chunks = key_width // HEAD
    groups = n // 4
    total = slots * tok
    bf, f32 = jnp.bfloat16, jnp.float32
    any_spec = pl.BlockSpec(memory_space=pl.ANY)
    vmem_spec = pl.BlockSpec(memory_space=pltpu.VMEM)
    dma = pltpu.SemaphoreType.DMA
    return pl.pallas_call(
        functools.partial(kernel, n),
        out_shape=jax.ShapeDtypeStruct(queries.shape, bf),
        in_specs=[any_spec, any_spec, vmem_spec, any_spec, any_spec, vmem_spec],
        out_specs=any_spec,
        scratch_shapes=[
            pltpu.VMEM((slots, tok, depth), bf),
            pltpu.VMEM(queries.shape[1:], bf),
            pltpu.VMEM(queries.shape[1:], bf),
            pltpu.VMEM((chunks, groups, 2, rows, 2 * HEAD), bf),
            pltpu.VMEM((groups, 2 * total, 2 * rows), bf),
            pltpu.VMEM((groups, total, 2 * rows), bf),
            pltpu.VMEM((chunks, total, 2 * HEAD), f32),
            pltpu.VMEM((chunks, total, 2 * HEAD), f32),
            pltpu.VMEM((chunks, total, 2 * HEAD), f32),
            pltpu.VMEM((chunks, total, 2 * HEAD), bf),
            pltpu.VMEM((chunks, total, 2 * HEAD), bf),
            pltpu.VMEM((slots, tok, HEAD), jnp.int32),
            dma((chunks, 2)), dma((slots,)), dma, dma((chunks,)),
            dma((chunks, groups)), dma((chunks, groups)),
            dma((chunks, groups)), dma((chunks, groups)),
            dma((slots, groups)), dma((slots, groups)),
            dma((chunks,)), dma((chunks,)), dma((chunks,)), dma((chunks,)),
        ],
        compiler_params=pltpu.CompilerParams(
            collective_id=0, has_side_effects=True, vmem_limit_bytes=60 * 1024 * 1024
        ),
    )(tokens, queries, gains, key_weight, value_weight, lengths)


def solution(mesh):
    return jax.shard_map(
        body,
        mesh=mesh,
        in_specs=(
            P("section", None, "fsdp", None),
            P("section", None, "fsdp", None),
            P("section", None),
            P("section", "fsdp", None),
            P("section", "fsdp", None),
            P(),
        ),
        out_specs=P("section", None, "fsdp", None),
        check_vma=False,
    )
```

```python
import functools

import jax
import jax.numpy as jnp
from jax import lax
from jax.experimental import pallas as pl
from jax.experimental.pallas import tpu as pltpu
from jax.sharding import PartitionSpec as P

HEAD = 128
AXIS = "fsdp"


def kernel(
    n,
    x_hbm, q_hbm, gain_ref, kw_hbm, vw_hbm, len_ref, o_hbm,
    x_v, q_v, o_v, wbuf, xs, sx, pk_s, pk_r, pv_s, pv_r, own_acc, kv, prior, start_s,
    lw_sem, lx_sem, lq_sem, lo_sem,
    ws_sem, wr_sem, ys_sem, yr_sem, xs_sem, xr_sem, ps_sem, pr_sem, ks_sem, kr_sem,
):
    slots, tok, depth = x_v.shape
    chunks, groups, _, rows, _ = wbuf.shape
    wide = 2 * rows
    total = slots * tok
    q_per_kv = q_v.shape[2] // (chunks * HEAD)
    me = lax.axis_index(AXIS)
    bit = me % 2
    cls = (me // 2) % 2
    grp = me // 4
    y_peer = me + 1 - 2 * bit
    z_peer = me + 2 - 4 * cls
    right = lax.rem(me + 1, n)
    left = lax.rem(me + n - 1, n)
    others = [lax.rem(grp + d, groups) for d in range(1, groups)]

    def dev(g):
        return g * 4 + cls * 2 + bit

    def load_w(c):
        cols = pl.ds(c * HEAD, HEAD)
        return [
            pltpu.make_async_copy(
                w.at[0, :, cols], wbuf.at[c, grp, bit, :, pl.ds(i * HEAD, HEAD)], lw_sem.at[c, i]
            )
            for i, w in enumerate((kw_hbm, vw_hbm))
        ]

    x_loads = [pltpu.make_async_copy(x_hbm.at[0, s], x_v.at[s], lx_sem.at[s]) for s in range(slots)]
    q_load = pltpu.make_async_copy(q_hbm.at[0], q_v, lq_sem)
    w_loads = [load_w(c) for c in range(chunks)]
    for copy in w_loads[0] + x_loads:
        copy.start()
    for c in range(1, chunks):
        for copy in w_loads[c]:
            copy.start()
    q_load.start()

    prior[...] = jnp.zeros_like(prior)

    barrier = pltpu.get_barrier_semaphore()
    peers = [y_peer, z_peer, right, left] + [dev(g) for g in others]
    for peer in peers:
        pl.semaphore_signal(barrier, inc=1, device_id={AXIS: peer}, device_id_type=pl.DeviceIdType.MESH)
    pl.semaphore_wait(barrier, len(peers))

    def remote(src, dst, send, recv, peer):
        return pltpu.make_async_remote_copy(
            src_ref=src, dst_ref=dst, send_sem=send, recv_sem=recv,
            device_id={AXIS: peer}, device_id_type=pl.DeviceIdType.MESH,
        )

    def w_copy(c, source_grp, index_grp, peer):
        block = wbuf.at[c, source_grp, bit]
        return remote(block, block, ws_sem.at[c, index_grp], wr_sem.at[c, source_grp], peer)

    def y_copy(c, g, side):
        block = wbuf.at[c, g, side]
        return remote(block, block, ys_sem.at[c, g], yr_sem.at[c, g], y_peer)

    outer = cls == grp % 2

    def send_w(c):
        for copy in w_loads[c]:
            copy.wait()
        for g in others:
            w_copy(c, grp, g, dev(g)).start()
        y_copy(c, grp, bit).start()

    def x_copy(s, g):
        return remote(
            sx.at[g, pl.ds(s * tok, tok)], xs.at[g, pl.ds(total + s * tok, tok)],
            xs_sem.at[s, g], xr_sem.at[s, g], z_peer,
        )

    def p_copies(c):
        return [
            remote(src.at[c], dst.at[c], ps_sem.at[c, i], pr_sem.at[c, i], z_peer)
            for i, (src, dst) in enumerate(((pk_s, pk_r), (pv_s, pv_r)))
        ]

    def k_copy(c):
        return remote(kv.at[c], prior.at[c], ks_sem.at[c], kr_sem.at[c], right)

    @pl.when(jnp.logical_not(outer))
    def _():
        send_w(0)

    block_rows = 16

    def norm_block(s, r):
        here = pl.ds(pl.multiple_of(r * block_rows, block_rows), block_rows)
        there = pl.ds(pl.multiple_of(s * tok + r * block_rows, block_rows), block_rows)
        squares = jnp.zeros((block_rows, 1), jnp.float32)
        step = 2 * wide
        for i in range(depth // step):
            piece = x_v[s, here, i * step:(i + 1) * step].astype(jnp.float32)
            squares = squares + jnp.sum(piece * piece, axis=-1, keepdims=True)
        inverse = lax.rsqrt(squares / depth + 1e-05)
        for g in range(groups):
            for mine in (True, False):
                first = (4 * g + 2 * (cls if mine else 1 - cls)) * rows
                cols = pl.ds(pl.multiple_of(first, HEAD), wide)
                value = x_v[s, here, cols].astype(jnp.float32) * inverse
                value = (value * gain_ref[0:1, cols].astype(jnp.float32)).astype(jnp.bfloat16)
                if mine:
                    xs[g, there, :] = value
                else:
                    sx[g, there, :] = value

    for s in range(slots):
        x_loads[s].wait()

        def norm_step(r, carry, s=s):
            norm_block(s, r)
            return carry

        lax.fori_loop(0, tok // block_rows, norm_step, 0)
        @pl.when(outer)
        def _(s=s):
            for g in range(groups):
                x_copy(s, g).start()

    @pl.when(outer)
    def _():
        send_w(0)

    for c in range(1, chunks):
        send_w(c)

    docs = len_ref.shape[1]
    rowi = lax.broadcasted_iota(jnp.int32, (docs, docs), 0)
    coli = lax.broadcasted_iota(jnp.int32, (docs, docs), 1)
    pos = lax.broadcasted_iota(jnp.int32, (tok, 1), 0) + me * tok
    for s in range(slots):
        lens = jnp.broadcast_to(len_ref[s:s + 1, :], (docs, docs))
        bounds = jnp.sum(jnp.where(coli <= rowi, lens, 0), axis=1, keepdims=True)
        bound_row = jnp.sum(jnp.where(coli == rowi, bounds, 0), axis=0, keepdims=True)
        start = jnp.max(jnp.where(bound_row <= pos, bound_row, 0), axis=1, keepdims=True)
        start_s[s] = jnp.broadcast_to(start, (tok, HEAD))
    q_load.wait()

    @pl.when(jnp.logical_not(outer))
    def _():
        for c in range(chunks):
            for g in others:
                w_copy(c, grp, g, dev(g)).wait_send()
        for s in range(slots):
            for g in range(groups):
                x_copy(s, g).start()

    def forward(c):
        for g in others:
            w_copy(c, g, g, dev(g)).wait_recv()
            y_copy(c, g, bit).start()

    def project(c, lo):
        acc = jnp.zeros((total, 2 * HEAD), jnp.float32)
        for g in range(groups):
            acc = acc + jnp.dot(
                xs[g, lo:lo + total, :], wbuf[c, g].reshape(wide, 2 * HEAD),
                preferred_element_type=jnp.float32,
            )
        return acc

    def own_rows(c):
        own_acc[c] = project(c, 0)

    def y_wait(c):
        for g in range(groups):
            y_copy(c, g, 1 - bit).wait_recv()

    @pl.when(outer)
    def _():
        for c in range(chunks):
            forward(c)
        for c in range(chunks):
            y_wait(c)
            own_rows(c)

    def stage_a(c):
        @pl.when(jnp.logical_not(outer))
        def _():
            if c == 0:
                forward(0)
            if c + 1 < chunks:
                forward(c + 1)
            y_wait(c)

        if c == 0:
            for s in range(slots):
                for g in range(groups):
                    x_copy(s, g).wait_recv()
        partial = project(c, total)
        pk_s[c] = partial[:, :HEAD]
        pv_s[c] = partial[:, HEAD:].astype(jnp.bfloat16)
        for copy in p_copies(c):
            copy.start()

        @pl.when(jnp.logical_not(outer))
        def _():
            own_rows(c)

    def stage_b(c):
        for copy in p_copies(c):
            copy.wait_recv()
        kv[c, :, 0:HEAD] = (own_acc[c, :, 0:HEAD] + pk_r[c]).astype(jnp.bfloat16)
        kv[c, :, HEAD:] = (own_acc[c, :, HEAD:] + pv_r[c].astype(jnp.float32)).astype(jnp.bfloat16)

        @pl.when(me < n - 1)
        def _():
            k_copy(c).start()

    key_pos = lax.broadcasted_iota(jnp.int32, (tok, 2 * tok), 1) + (me - 1) * tok
    query_pos = lax.broadcasted_iota(jnp.int32, (tok, 2 * tok), 0) + me * tok

    def out_copy(c):
        cols = pl.ds(c * q_per_kv * HEAD, q_per_kv * HEAD)
        return pltpu.make_async_copy(o_v.at[:, :, cols], o_hbm.at[0, :, :, cols], lo_sem.at[c])

    def stage_c(c):
        @pl.when(me > 0)
        def _():
            k_copy(c).wait_recv()

        for s in range(slots):
            here = slice(s * tok, (s + 1) * tok)
            keys = jnp.concatenate([prior[c, here, 0:HEAD], kv[c, here, 0:HEAD]], axis=0)
            values = jnp.concatenate([prior[c, here, HEAD:], kv[c, here, HEAD:]], axis=0)
            allowed = (key_pos >= start_s[s][:, 0:1]) & (key_pos <= query_pos)

            def head_step(h, carry, s=s, keys=keys, values=values, allowed=allowed):
                cols = pl.ds(pl.multiple_of((c * q_per_kv + h) * HEAD, HEAD), HEAD)
                scores = lax.dot_general(
                    q_v[s, :, cols], keys, (((1,), (1,)), ((), ())),
                    preferred_element_type=jnp.float32,
                ) * HEAD ** (-0.5)
                scores = jnp.where(allowed, scores, -1e30)
                maxima = jnp.max(scores, axis=-1, keepdims=True)
                exponent = jnp.where(allowed, jnp.exp(scores - maxima), 0.0)
                sums = jnp.sum(exponent, axis=-1, keepdims=True)
                soft = (exponent / sums).astype(jnp.bfloat16)
                mixed = jnp.dot(soft, values, preferred_element_type=jnp.float32)
                o_v[s, :, cols] = mixed.astype(jnp.bfloat16)
                return carry

            lax.fori_loop(0, q_per_kv, head_step, 0, unroll=True)
        out_copy(c).start()

    for c in range(chunks - 1):
        stage_a(c)
    stage_b(0)
    stage_b(1)
    stage_a(chunks - 1)
    for c in range(2, chunks):
        stage_c(c - 2)
        stage_b(c)
    stage_c(chunks - 2)
    stage_c(chunks - 1)

    for c in range(chunks):
        out_copy(c).wait()
        @pl.when(outer)
        def _(c=c):
            for g in others:
                w_copy(c, grp, g, dev(g)).wait_send()

        for g in range(groups):
            y_copy(c, g, bit).wait_send()
        for copy in p_copies(c):
            copy.wait_send()

        @pl.when(me < n - 1)
        def _(c=c):
            k_copy(c).wait_send()

    for s in range(slots):
        for g in range(groups):
            x_copy(s, g).wait_send()


def body(tokens, queries, gains, key_weight, value_weight, lengths):
    n = lax.axis_size(AXIS)
    _, slots, tok, depth = tokens.shape
    _, rows, key_width = key_weight.shape
    chunks = key_width // HEAD
    groups = n // 4
    total = slots * tok
    bf, f32 = jnp.bfloat16, jnp.float32
    any_spec = pl.BlockSpec(memory_space=pl.ANY)
    vmem_spec = pl.BlockSpec(memory_space=pltpu.VMEM)
    dma = pltpu.SemaphoreType.DMA
    return pl.pallas_call(
        functools.partial(kernel, n),
        out_shape=jax.ShapeDtypeStruct(queries.shape, bf),
        in_specs=[any_spec, any_spec, vmem_spec, any_spec, any_spec, vmem_spec],
        out_specs=any_spec,
        scratch_shapes=[
            pltpu.VMEM((slots, tok, depth), bf),
            pltpu.VMEM(queries.shape[1:], bf),
            pltpu.VMEM(queries.shape[1:], bf),
            pltpu.VMEM((chunks, groups, 2, rows, 2 * HEAD), bf),
            pltpu.VMEM((groups, 2 * total, 2 * rows), bf),
            pltpu.VMEM((groups, total, 2 * rows), bf),
            pltpu.VMEM((chunks, total, HEAD), f32),
            pltpu.VMEM((chunks, total, HEAD), f32),
            pltpu.VMEM((chunks, total, HEAD), bf),
            pltpu.VMEM((chunks, total, HEAD), bf),
            pltpu.VMEM((chunks, total, 2 * HEAD), f32),
            pltpu.VMEM((chunks, total, 2 * HEAD), bf),
            pltpu.VMEM((chunks, total, 2 * HEAD), bf),
            pltpu.VMEM((slots, tok, HEAD), jnp.int32),
            dma((chunks, 2)), dma((slots,)), dma, dma((chunks,)),
            dma((chunks, groups)), dma((chunks, groups)),
            dma((chunks, groups)), dma((chunks, groups)),
            dma((slots, groups)), dma((slots, groups)),
            dma((chunks, 2)), dma((chunks, 2)), dma((chunks,)), dma((chunks,)),
        ],
        compiler_params=pltpu.CompilerParams(
            collective_id=0, has_side_effects=True, vmem_limit_bytes=60 * 1024 * 1024
        ),
    )(tokens, queries, gains, key_weight, value_weight, lengths)


def solution(mesh):
    return jax.shard_map(
        body,
        mesh=mesh,
        in_specs=(
            P("section", None, "fsdp", None),
            P("section", None, "fsdp", None),
            P("section", None),
            P("section", "fsdp", None),
            P("section", "fsdp", None),
            P(),
        ),
        out_specs=P("section", None, "fsdp", None),
        check_vma=False,
    )
```
